512 devices in a mesh: cells: 128 (over y, x, z_lo, core), obs: 4 (over z_hi).
Axes of the slice: x: 4, y: 8, z: 8 (z_hi: 4, z_lo: 2; z = z_hi * 2 + z_lo), core: 2. Of those that a mesh axis runs over, the one named last changes fastest.
Arguments:
- histories: bfloat16 [64, 384], P('obs'), may hold values from -6 to 6
- amplitude: bfloat16 [64, 5, 131072], P('obs', None, 'cells'), may hold values from -0.75 to 0.75
- weights: bfloat16 [131072, 256], P('cells'), may hold values from -0.375 to 0.375
- retarded: int32 [64, 1024], P('obs', 'cells'), may hold values from 0 to 128
- owner_block: int32 [131072], P('cells'), may hold values from 0 to 127, as said below
- owner_cell: int32 [131072], P('cells'), may hold values from 0 to 16383
- adjoint: float32 [5, 256, 64, 128], P(None, 'cells', 'obs'), may hold values from -6 to 6
- step_size: float32 [256, 64, 128], P('cells', 'obs'), may hold values from 0.1 to 0.6
- jacobian: float32 [128, 3, 5, 5], P('cells'), may hold values from -6 to 6
Outputs:
- adjoint_next: float32 [5, 256, 64, 128], P(None, 'cells', 'obs')
- panel_source: float32 [5, 131072], P(None, 'cells')
The draws below stay inside these ranges and needn't reach their ends.
Inputs may be any that keep to these rules, and one draw needn't show every extreme that they name: `owner_block`: among each device's 1024 panels at most 32 name one owner block; one owner block, drawn from the seed, is named by exactly 32 panels of every device.
All inputs are finite; a program needn't handle non-finite values.
Results may differ from the reference program's by a relative error of at most 0.0003.
Values sent between devices are 32-bit elements; how exact they have to be, the bound alone decides.
No kernel may reach another device: no remote copies, remote signals or barrier semaphores. Data moves between devices by JAX's collectives and lax.ppermute only.
A program may use at most 192 MiB of HBM per device.

```python
import math
import jax
import jax.numpy as jnp
from jax import lax

NOBS = 64
SAMPLES = 256
SPAN = 128
COMP = 5
TILE = 128
PAN_DEV = 1024
AZ_DEV = 2
NZ = 128
HIST = 384
CAP = 32
PANELS = 131072
TILES = 1024
NA = 256
NR = 64
BLOCK_CELLS = 16384
N_CELLS = 128


def draw_owner_block(key, part):
    folded = jax.random.fold_in(key, 7)
    first_key, shift_key, order_key = jax.random.split(folded, 3)
    crowded = jax.random.randint(first_key, (), 0, N_CELLS)
    shifts = jax.random.randint(shift_key, (N_CELLS, 1), 0, N_CELLS - 1)
    within = jnp.arange(PAN_DEV, dtype=jnp.int32)[None, :]
    others = (crowded + 1 + (within - CAP + shifts) % (N_CELLS - 1)) % N_CELLS
    blocks = jnp.where(within < CAP, crowded, others)

    def shuffle(block_key):
        return jax.random.permutation(block_key, PAN_DEV)
    orders = jax.vmap(shuffle)(jax.random.split(order_key, N_CELLS))
    shuffled = jnp.take_along_axis(blocks, orders, axis=1)
    return shuffled.reshape(PANELS).astype(jnp.int32)


def plant(entries, rng, low, largest):
    place = [jax.random.randint(jax.random.fold_in(rng, axis), (), 0, length) for axis, length in enumerate(entries.shape)]
    widest = entries.shape.index(max(entries.shape))
    next_to = place[:widest] + [(place[widest] + 1) % entries.shape[widest]] + place[widest + 1:]
    return entries.at[tuple(place)].set(low).at[tuple(next_to)].set(largest)


def level_of(stream_key, extent, shards, smallest, top_value):
    factor_of, own = 1.0, jax.random.fold_in(stream_key, 6)
    for position, blocks in shards:
        steps = jnp.exp(jax.random.uniform(jax.random.fold_in(own, position), (blocks,), jnp.float32, smallest / len(shards), top_value / len(shards)))
        factor_of = factor_of * jnp.repeat(steps, extent[position] // blocks).reshape([-1 if axis == position else 1 for axis in range(len(extent))])
    return factor_of


def gaussian(rng, extent, spread, most, cuts=(), kind=jnp.bfloat16):
    factor_of = level_of(rng, extent, cuts, -0.22, 0.18) if cuts else 1.0
    entries = jax.random.normal(rng, extent, jnp.float32) * spread * factor_of
    return jnp.minimum(jnp.maximum(entries, -most), most).astype(kind)


def setup_inputs(seed: int = 0) -> dict:
    streams_of = jax.random.split(jax.random.key(seed), 10)
    histories = gaussian(streams_of[0], (NOBS, HIST), 1.0, 6.0, ((0, 4),))
    amplitude = gaussian(streams_of[1], (NOBS, COMP, PANELS), NOBS ** -0.5, 0.75, ((0, 4), (2, 128)))
    weights = gaussian(streams_of[2], (PANELS, SAMPLES), SAMPLES ** -0.5, 0.375, ((0, 128),))
    retarded = plant(jax.random.randint(streams_of[3], (NOBS, TILES), 0, SPAN + 1), jax.random.fold_in(streams_of[3], 1), 0, SPAN).astype(jnp.int32)
    owner_block = draw_owner_block(jax.random.fold_in(streams_of[9], 71), 0)
    owner_cell = plant(jax.random.randint(streams_of[5], (PANELS,), 0, BLOCK_CELLS), jax.random.fold_in(streams_of[5], 1), 0, BLOCK_CELLS - 1).astype(jnp.int32)
    adjoint = gaussian(streams_of[6], (COMP, NA, NR, NZ), 1.0, 6.0, ((1, 128), (2, 4)), jnp.float32)
    step_size = jnp.clip(jnp.exp(math.log(0.6) - 1.7917595 * jax.random.uniform(streams_of[7], (NA, NR, NZ), jnp.float32) ** level_of(streams_of[7], (NA, NR, NZ), ((0, 128), (1, 4)), -0.2, 0.2)), 0.1, 0.6)
    jacobian = gaussian(streams_of[8], (N_CELLS, 3, COMP, COMP), 0.45, 6.0, ((0, 128),), jnp.float32)
    return dict(histories=histories, amplitude=amplitude, weights=weights, retarded=retarded, owner_block=owner_block, owner_cell=owner_cell, adjoint=adjoint, step_size=step_size, jacobian=jacobian)


smoothing = 0.25


def slide(series, offset):
    return lax.dynamic_slice_in_dim(series, offset, SAMPLES)


def reference(histories, amplitude, weights, retarded, owner_block, owner_cell, adjoint, step_size, jacobian):
    tile_count = PANELS // TILE
    weights_tiled = weights.reshape(tile_count, TILE, SAMPLES)
    amplitude_tiled = amplitude.reshape(NOBS, COMP, tile_count, TILE)

    def one_tile(tile_index):
        offsets = lax.dynamic_index_in_dim(retarded, tile_index, 1, keepdims=False)
        window = jax.vmap(slide)(histories, offsets)
        tiled = lax.dynamic_index_in_dim(weights_tiled, tile_index, 0, keepdims=False)
        projected = jnp.dot(tiled, window.T, preferred_element_type=jnp.float32)
        amps = lax.dynamic_index_in_dim(amplitude_tiled, tile_index, 2, keepdims=False).astype(jnp.float32)
        return jnp.sum(amps * projected.T[:, None, :], axis=0)

    sources = lax.map(one_tile, jnp.arange(tile_count, dtype=jnp.int32))
    panel_source = jnp.transpose(sources, (1, 0, 2)).reshape(COMP, PANELS)
    flat_index = owner_block * BLOCK_CELLS + owner_cell
    surface = jnp.zeros((COMP, NA * NR * NZ), jnp.float32).at[:, flat_index].add(panel_source)
    surface = surface.reshape(COMP, NA, NR, NZ)

    def rotate(direction, difference):
        reshaped = difference.reshape(COMP, N_CELLS, AZ_DEV, NR, NZ)
        rotated = jnp.einsum('bkc,kbarz->cbarz', jacobian[:, direction], reshaped, precision=lax.Precision.HIGHEST)
        return rotated.reshape(COMP, NA, NR, NZ)

    radial_pad = jnp.pad(adjoint, ((0, 0), (0, 0), (1, 1), (0, 0)))
    axial_pad = jnp.pad(adjoint, ((0, 0), (0, 0), (0, 0), (1, 1)))
    neighbours = (
        (jnp.roll(adjoint, -1, axis=1), jnp.roll(adjoint, 1, axis=1)),
        (radial_pad[:, :, 2:], radial_pad[:, :, :-2]),
        (axial_pad[..., 2:], axial_pad[..., :-2]),
    )
    summed = jnp.zeros_like(adjoint)
    for direction in range(3):
        forward, backward = neighbours[direction]
        summed = summed + (0.5 * rotate(direction, forward - backward) + smoothing * (forward - 2.0 * adjoint + backward))
    adjoint_next = adjoint + step_size[None] * summed + surface
    return (adjoint_next, panel_source)
```

```python
import jax
import jax.numpy as jnp
from jax import lax
from jax.experimental import pallas as pl
from jax.experimental.pallas import tpu as pltpu
from jax.sharding import PartitionSpec as P

TILE = 128
COMP = 5
CAP = 32
SMOOTHING = 0.25
F32 = jnp.float32
BF16 = jnp.bfloat16
NT = (((1,), (1,)), ((), ()))

VMEM = pl.BlockSpec(memory_space=pltpu.MemorySpace.VMEM)
SMEM = pl.BlockSpec(memory_space=pltpu.MemorySpace.SMEM)
ANY = pl.BlockSpec(memory_space=pl.ANY)


def iota(shape, dim):
    return lax.broadcasted_iota(jnp.int32, shape, dim)


def split(x):
    high = x.astype(BF16)
    return high, (x - high.astype(F32)).astype(BF16)


def project(hist_ref, amp_ref, weight_ref, ret_ref, adj_ref, out_ref):
    observers = hist_ref.shape[0]
    tiles = ret_ref.shape[1]
    hist = hist_ref[...].astype(F32)
    rows = tiles * observers
    column = [jnp.concatenate([hist[:, j * 128 : (j + 1) * 128]] * tiles, axis=0) for j in range(3)]
    shift = jnp.concatenate(
        [jnp.broadcast_to(ret_ref[:, t : t + 1], (observers, 128)) for t in range(tiles)], axis=0
    )
    lane = iota((rows, 128), 1)
    far = shift >= 128
    column = [
        jnp.where(far, column[1], column[0]),
        jnp.where(far, column[2], column[1]),
        column[2],
    ]
    for amount in (64, 32, 16, 8, 4, 2, 1):
        turned = [pltpu.roll(x, 128 - amount, 1) for x in column]
        stays = lane < 128 - amount
        chosen = (shift & amount) != 0
        column = [
            jnp.where(chosen, jnp.where(stays, turned[0], turned[1]), column[0]),
            jnp.where(chosen, jnp.where(stays, turned[1], turned[2]), column[1]),
            jnp.where(chosen, turned[2], column[2]),
        ]
    window = jnp.concatenate(column[:2], axis=1).astype(BF16)
    for t in range(tiles):
        span = slice(t * TILE, (t + 1) * TILE)
        projected = lax.dot_general(
            window[t * observers : (t + 1) * observers],
            weight_ref[span, :],
            NT,
            preferred_element_type=F32,
        )
        total = jnp.zeros((COMP, TILE), F32)
        for o in range(observers):
            total = total + amp_ref[o, :, span].astype(F32) * projected[o : o + 1, :]
        for copy in range(out_ref.shape[0]):
            out_ref[copy, :COMP, span] = total
    azimuths, radii = adj_ref.shape[1:3]
    place = 0
    for row in (0, radii - 1):
        for c in range(COMP):
            for a in range(azimuths):
                line = adj_ref[c, a, row : row + 1, :]
                where = (COMP + place // 8, place % 8 * 128)
                for copy in range(out_ref.shape[0]):
                    out_ref[copy, where[0] : where[0] + 1, where[1] : where[1] + 128] = line
                place += 1
    for rest in range(place, 24):
        for copy in range(out_ref.shape[0]):
            out_ref[copy, COMP + rest // 8 : COMP + rest // 8 + 1, rest % 8 * 128 : (rest % 8 + 1) * 128] = jnp.zeros(
                (1, 128), F32
            )


def radial_line(ref, group, side, c, a):
    place = side * 10 + c * 2 + a
    return ref[group, COMP + place // 8, pl.ds(place % 8 * 128, 128)].reshape(1, 128)


def order(after_ref, block_ref, adj_ref, rank_ref, head_ref, tail_ref):
    chunks, width = block_ref.shape
    blocks = 128
    head_ref[...] = adj_ref[:, 0]
    tail_ref[...] = adj_ref[:, adj_ref.shape[1] - 1]
    mark = jnp.where((iota((width, 2 * width), 0) < iota((width, 2 * width), 1)), 1.0, 0.0).astype(BF16)
    before = jnp.zeros((blocks, width), F32)
    for j in range(chunks):
        same = iota((blocks, width), 0) == block_ref[j : j + 1, :]
        counted = jnp.dot(jnp.where(same, 1.0, 0.0).astype(BF16), mark, preferred_element_type=F32)
        rank_ref[j : j + 1, :] = jnp.sum(
            jnp.where(same, counted[:, :width] + before, 0.0), axis=0, keepdims=True
        )
        before = before + counted[:, width:]


def pack(part_ref, block_ref, cell_ref, rank_ref, source_ref, out_ref):
    chunks, width = block_ref.shape
    source = part_ref[0, :COMP, :]
    for group in range(1, part_ref.shape[0]):
        source = source + part_ref[group, :COMP, :]
    source_ref[...] = source
    total = jnp.zeros((128, (COMP + 1) * CAP), F32)
    for j in range(chunks):
        span = slice(j * width, (j + 1) * width)
        slot = iota((CAP, width), 0).astype(F32) == rank_ref[j : j + 1, :]
        same = jnp.where(iota((128, width), 0) == block_ref[j : j + 1, :], 1.0, 0.0).astype(BF16)
        lines = [source[c : c + 1, span] for c in range(COMP)] + [cell_ref[j : j + 1, :].astype(F32)]
        placed = jnp.concatenate([jnp.where(slot, line, 0.0) for line in lines], axis=0)
        high, low = split(placed)
        total = (
            total
            + lax.dot_general(same, high, NT, preferred_element_type=F32)
            + lax.dot_general(same, low, NT, preferred_element_type=F32)
        )
    out_ref[:, :128] = total[:, :128]
    out_ref[:, 128:] = jnp.concatenate([total[:, 128:], jnp.zeros((128, 64), F32)], axis=1)


def stencil(part_ref, next_ref, prev_ref, adj_ref, step_ref, jac_ref, out_ref):
    group = lax.axis_index("obs")
    groups = part_ref.shape[0]
    azimuths, radii, length = adj_ref.shape[1:]
    row = iota((radii, length), 0)
    lane = iota((radii, length), 1)
    below = jnp.maximum(group - 1, 0)
    above = jnp.minimum(group + 1, groups - 1)
    has_below = jnp.where(group > 0, 1.0, 0.0)
    has_above = jnp.where(group < groups - 1, 1.0, 0.0)
    for a in range(azimuths):
        centre = [adj_ref[c, a] for c in range(COMP)]
        pairs = [[], [], []]
        for c in range(COMP):
            x = centre[c]
            ahead = next_ref[c] if a == azimuths - 1 else adj_ref[c, a + 1]
            behind = prev_ref[c] if a == 0 else adj_ref[c, a - 1]
            pairs[0].append((ahead, behind))
            upper = radial_line(part_ref, above, 0, c, a) * has_above
            lower = radial_line(part_ref, below, 1, c, a) * has_below
            pairs[1].append(
                (
                    jnp.where(row == radii - 1, upper, pltpu.roll(x, radii - 1, 0)),
                    jnp.where(row == 0, lower, pltpu.roll(x, 1, 0)),
                )
            )
            pairs[2].append(
                (
                    jnp.where(lane == length - 1, 0.0, pltpu.roll(x, length - 1, 1)),
                    jnp.where(lane == 0, 0.0, pltpu.roll(x, 1, 1)),
                )
            )
        differences = [[f - b for f, b in pairs[d]] for d in range(3)]
        for c in range(COMP):
            rotated = jnp.zeros((radii, length), F32)
            spread = -6.0 * centre[c]
            for d in range(3):
                spread = spread + (pairs[d][c][0] + pairs[d][c][1])
                for k in range(COMP):
                    rotated = rotated + jac_ref[0, d, k, c] * differences[d][k]
            summed = 0.5 * rotated + SMOOTHING * spread
            out_ref[c, a] = centre[c] + step_ref[a] * summed


def land(got_ref, base_ref, out_ref):
    group = lax.axis_index("obs")
    azimuths, radii, length = base_ref.shape[1:]
    radii_all = radii * lax.axis_size("obs")
    local_rows = azimuths * radii
    got = jnp.concatenate([got_ref[:, :128].T, got_ref[:, 128:].T], axis=0)
    sources = got_ref.shape[0]
    high, low = split(got)
    high, low = high.astype(F32), low.astype(F32)
    cell = got[COMP * CAP : (COMP + 1) * CAP].astype(jnp.int32)
    cell_row = cell >> 7
    cell_lane = cell & 127
    local = iota((local_rows, sources), 0)
    wanted = (local // radii) * radii_all + local % radii + group * radii
    total = jnp.zeros((COMP * local_rows, length), F32)
    for first in range(0, CAP, 2):
        highs, lows, lanes = [], [], []
        for k in (first, first + 1):
            here = wanted == cell_row[k : k + 1]
            highs.append(
                jnp.concatenate([jnp.where(here, high[c * CAP + k : c * CAP + k + 1], 0.0) for c in range(COMP)], axis=0).astype(BF16)
            )
            lows.append(
                jnp.concatenate([jnp.where(here, low[c * CAP + k : c * CAP + k + 1], 0.0) for c in range(COMP)], axis=0).astype(BF16)
            )
            lanes.append(jnp.where(iota((length, sources), 0) == cell_lane[k : k + 1], 1.0, 0.0).astype(BF16))
        at = jnp.concatenate(lanes, axis=1)
        total = (
            total
            + lax.dot_general(jnp.concatenate(highs, axis=1), at, NT, preferred_element_type=F32)
            + lax.dot_general(jnp.concatenate(lows, axis=1), at, NT, preferred_element_type=F32)
        )
    for c in range(COMP):
        for a in range(azimuths):
            start = (c * azimuths + a) * radii
            out_ref[c, a] = base_ref[c, a] + total[start : start + radii]


def on_device(
    histories, amplitude, weights, retarded, owner_block, owner_cell, adjoint, step_size, jacobian
):
    groups = lax.axis_size("obs")
    count = lax.axis_size("cells")
    panels = weights.shape[0]
    blocks2 = owner_block.reshape(panels // 128, 128)
    cells2 = owner_cell.reshape(panels // 128, 128)
    shape = jax.ShapeDtypeStruct

    partial_copies = pl.pallas_call(
        project,
        out_shape=shape((groups, 8, panels), F32),
        in_specs=[VMEM] * 5,
        out_specs=VMEM,
        name="project",
    )(histories, amplitude, weights, retarded, adjoint)
    parts = lax.all_to_all(partial_copies, "obs", split_axis=0, concat_axis=0, tiled=True)

    edge = shape((COMP,) + adjoint.shape[2:], F32)
    rank, head, tail = pl.pallas_call(
        order,
        out_shape=(shape(blocks2.shape, F32), edge, edge),
        in_specs=[ANY, VMEM, VMEM],
        out_specs=(VMEM, VMEM, VMEM),
        name="order",
    )(partial_copies, blocks2, adjoint)
    panel_source, outgoing = pl.pallas_call(
        pack,
        out_shape=(shape((COMP, panels), F32), shape((count, 256), F32)),
        in_specs=[VMEM] * 4,
        out_specs=(VMEM, VMEM),
        name="pack",
    )(parts, blocks2, cells2, rank)
    received = lax.all_to_all(outgoing, "cells", split_axis=0, concat_axis=0, tiled=True)

    behind = lax.ppermute(tail, "cells", [(i, (i + 1) % count) for i in range(count)])
    ahead = lax.ppermute(head, "cells", [((i + 1) % count, i) for i in range(count)])
    base = pl.pallas_call(
        stencil,
        out_shape=shape(adjoint.shape, F32),
        in_specs=[VMEM] * 5 + [SMEM],
        out_specs=VMEM,
        name="stencil",
    )(parts, ahead, behind, adjoint, step_size, jacobian)
    adjoint_next = pl.pallas_call(
        land,
        out_shape=shape(adjoint.shape, F32),
        in_specs=[VMEM] * 2,
        out_specs=VMEM,
        name="land",
    )(received, base)
    return adjoint_next, panel_source


def solution(mesh):
    return jax.shard_map(
        on_device,
        mesh=mesh,
        in_specs=(
            P("obs", None),
            P("obs", None, "cells"),
            P("cells", None),
            P("obs", "cells"),
            P("cells"),
            P("cells"),
            P(None, "cells", "obs", None),
            P("cells", "obs", None),
            P("cells", None, None, None),
        ),
        out_specs=(P(None, "cells", "obs", None), P(None, "cells")),
        check_vma=False,
    )
```

```python
import jax
import jax.numpy as jnp
from jax import lax
from jax.experimental import pallas as pl
from jax.experimental.pallas import tpu as pltpu
from jax.sharding import PartitionSpec as P

TILE = 128
COMP = 5
CAP = 32
SMOOTHING = 0.25
F32 = jnp.float32
BF16 = jnp.bfloat16
NT = (((1,), (1,)), ((), ()))

VMEM = pl.BlockSpec(memory_space=pltpu.MemorySpace.VMEM)
SMEM = pl.BlockSpec(memory_space=pltpu.MemorySpace.SMEM)
ANY = pl.BlockSpec(memory_space=pl.ANY)


def iota(shape, dim):
    return lax.broadcasted_iota(jnp.int32, shape, dim)


def project(hist_ref, ret_ref, amp_hbm, weight_hbm, adj_hbm, out_ref, head_ref, tail_ref, amp_ref, weight_ref, adj_ref, sems):
    moves = [
        pltpu.make_async_copy(source, target, sems.at[i])
        for i, (source, target) in enumerate(((weight_hbm, weight_ref), (amp_hbm, amp_ref), (adj_hbm, adj_ref)))
    ]
    for move in moves:
        move.start()
    group = lax.axis_index("obs")
    observers = hist_ref.shape[0]
    tiles = ret_ref.shape[0]
    hist = hist_ref[...].astype(F32)
    rows = tiles * observers
    column = [jnp.concatenate([hist[:, j * 128 : (j + 1) * 128]] * tiles, axis=0) for j in range(3)]
    eye = iota((observers, observers), 0) == iota((observers, observers), 1)
    shift = jnp.concatenate(
        [
            jnp.broadcast_to(
                jnp.sum(jnp.where(eye, ret_ref[t : t + 1, :].astype(F32), 0.0), axis=1, keepdims=True), (observers, 128)
            )
            for t in range(tiles)
        ],
        axis=0,
    ).astype(jnp.int32)
    lane = iota((rows, 128), 1)
    far = shift >= 128
    column = [
        jnp.where(far, column[1], column[0]),
        jnp.where(far, column[2], column[1]),
        column[2],
    ]
    for amount in (64, 32, 16, 8, 4, 2, 1):
        turned = [pltpu.roll(x, 128 - amount, 1) for x in column]
        stays = lane < 128 - amount
        chosen = (shift & amount) != 0
        column = [
            jnp.where(chosen, jnp.where(stays, turned[0], turned[1]), column[0]),
            jnp.where(chosen, jnp.where(stays, turned[1], turned[2]), column[1]),
            jnp.where(chosen, turned[2], column[2]),
        ]
    window = jnp.concatenate(column[:2], axis=1).astype(BF16)
    for move in moves:
        move.wait()
    copies = out_ref.shape[0]
    for t in range(tiles):
        span = slice(t * TILE, (t + 1) * TILE)
        projected = lax.dot_general(
            window[t * observers : (t + 1) * observers],
            weight_ref[span, :],
            NT,
            preferred_element_type=F32,
        )
        for c in range(COMP):
            total = jnp.sum(amp_ref[c, :, span].astype(F32) * projected, axis=0, keepdims=True)
            for copy in range(copies):
                out_ref[copy, c * tiles + t : c * tiles + t + 1, :] = total
    azimuths, radii = adj_ref.shape[1:3]
    head_ref[...] = adj_ref[:, 0]
    tail_ref[...] = adj_ref[:, azimuths - 1]
    for c in range(COMP):
        for a in range(azimuths):
            place = COMP * tiles + c * azimuths + a
            for copy in range(copies):
                up = jnp.full((1, 128), copy, jnp.int32) > group
                out_ref[copy, place : place + 1, :] = jnp.where(
                    up, adj_ref[c, a, radii - 1 : radii, :], adj_ref[c, a, 0:1, :]
                )
    for copy in range(copies):
        out_ref[copy, 50:56, :] = jnp.zeros((6, 128), F32)


def order(after_ref, block_ref, same_ref, slot_ref):
    chunks, width = block_ref.shape
    blocks = 128
    mark = jnp.where((iota((width, 2 * width), 0) < iota((width, 2 * width), 1)), 1.0, 0.0).astype(BF16)
    before = jnp.zeros((blocks, width), F32)
    for j in range(chunks):
        same = iota((blocks, width), 0) == block_ref[j : j + 1, :]
        marked = jnp.where(same, 1.0, 0.0).astype(BF16)
        same_ref[j] = marked
        counted = jnp.dot(marked, mark, preferred_element_type=F32)
        rank = jnp.sum(jnp.where(same, counted[:, :width] + before, 0.0), axis=0, keepdims=True)
        slot_ref[j] = jnp.where(iota((CAP, width), 0).astype(F32) == rank, 1.0, 0.0).astype(BF16)
        before = before + counted[:, width:]


def pack(part_ref, same_ref, slot_ref, cell_ref, source_ref, out_ref):
    chunks, width = cell_ref.shape
    count = COMP * chunks
    source = part_ref[0, :count, :]
    for group in range(1, part_ref.shape[0]):
        source = source + part_ref[group, :count, :]
    for c in range(COMP):
        for j in range(chunks):
            source_ref[c : c + 1, j * width : (j + 1) * width] = source[c * chunks + j : c * chunks + j + 1, :]
    lines = jnp.concatenate([source, cell_ref[...].astype(F32)], axis=0)
    high = lines.astype(BF16).astype(F32)
    low = lines - high
    total = jnp.zeros((128, (COMP + 1) * CAP), F32)
    for j in range(chunks):
        slot = slot_ref[j]
        placed = []
        for part in (high, low):
            placed.append(
                jnp.concatenate(
                    [
                        jnp.broadcast_to(part[c * chunks + j : c * chunks + j + 1, :], (CAP, width)).astype(BF16) * slot
                        for c in range(COMP + 1)
                    ],
                    axis=0,
                )
            )
        same = same_ref[j]
        total = total + lax.dot_general(
            jnp.concatenate([same, same], axis=1),
            jnp.concatenate(placed, axis=1),
            NT,
            preferred_element_type=F32,
        )
    out_ref[:, :128] = total[:, :128]
    out_ref[:, 128:] = jnp.concatenate([total[:, 128:], jnp.zeros((128, 64), F32)], axis=1)


def stencil(part_ref, next_ref, prev_ref, adj_ref, step_ref, jac_ref, out_ref):
    group = lax.axis_index("obs")
    groups = part_ref.shape[0]
    azimuths, radii, length = adj_ref.shape[1:]
    row = iota((radii, length), 0)
    lane = iota((radii, length), 1)
    below = jnp.maximum(group - 1, 0)
    above = jnp.minimum(group + 1, groups - 1)
    has_below = jnp.where(group > 0, 1.0, 0.0)
    has_above = jnp.where(group < groups - 1, 1.0, 0.0)
    uppers = part_ref[above, 40:56, :] * has_above
    lowers = part_ref[below, 40:56, :] * has_below
    for a in range(azimuths):
        centre = [adj_ref[c, a] for c in range(COMP)]
        pairs = [[], [], []]
        for c in range(COMP):
            x = centre[c]
            ahead = next_ref[c] if a == azimuths - 1 else adj_ref[c, a + 1]
            behind = prev_ref[c] if a == 0 else adj_ref[c, a - 1]
            pairs[0].append((ahead, behind))
            place = c * azimuths + a
            upper = uppers[place : place + 1]
            lower = lowers[place : place + 1]
            pairs[1].append(
                (
                    jnp.where(row == radii - 1, upper, pltpu.roll(x, radii - 1, 0)),
                    jnp.where(row == 0, lower, pltpu.roll(x, 1, 0)),
                )
            )
            pairs[2].append(
                (
                    jnp.where(lane == length - 1, 0.0, pltpu.roll(x, length - 1, 1)),
                    jnp.where(lane == 0, 0.0, pltpu.roll(x, 1, 1)),
                )
            )
        differences = [[f - b for f, b in pairs[d]] for d in range(3)]
        for c in range(COMP):
            rotated = jnp.zeros((radii, length), F32)
            spread = -6.0 * centre[c]
            for d in range(3):
                spread = spread + (pairs[d][c][0] + pairs[d][c][1])
                for k in range(COMP):
                    rotated = rotated + jac_ref[d, k, 0, c] * differences[d][k]
            summed = 0.5 * rotated + SMOOTHING * spread
            out_ref[c, a] = centre[c] + step_ref[a] * summed


def land(got_ref, base_ref, out_ref):
    group = lax.axis_index("obs")
    azimuths, radii, length = base_ref.shape[1:]
    radii_all = radii * lax.axis_size("obs")
    local_rows = azimuths * radii
    got = jnp.concatenate([got_ref[:, :128].T, got_ref[:, 128:].T], axis=0)
    sources = got_ref.shape[0]
    high = got.astype(BF16).astype(F32)
    low = got - high
    cell = got[COMP * CAP : (COMP + 1) * CAP].astype(jnp.int32)
    cell_row = cell >> 7
    cell_lane = cell & 127
    local = iota((local_rows, sources), 0)
    wanted = (local // radii) * radii_all + local % radii + group * radii
    total = jnp.zeros((2 * COMP * local_rows, length), F32)
    for first in range(0, CAP, 2):
        values, lanes = [], []
        for k in (first, first + 1):
            here = jnp.where(wanted == cell_row[k : k + 1], 1.0, 0.0).astype(BF16)
            values.append(
                jnp.concatenate(
                    [
                        jnp.broadcast_to(part[c * CAP + k : c * CAP + k + 1], (local_rows, sources)).astype(BF16) * here
                        for part in (high, low)
                        for c in range(COMP)
                    ],
                    axis=0,
                )
            )
            lanes.append(jnp.where(iota((length, sources), 0) == cell_lane[k : k + 1], 1.0, 0.0).astype(BF16))
        total = total + lax.dot_general(
            jnp.concatenate(values, axis=1), jnp.concatenate(lanes, axis=1), NT, preferred_element_type=F32
        )
    half = COMP * local_rows
    for c in range(COMP):
        for a in range(azimuths):
            start = (c * azimuths + a) * radii
            out_ref[c, a] = base_ref[c, a] + (total[start : start + radii] + total[half + start : half + start + radii])


def near(x):
    return pltpu.with_memory_space_constraint(x, pltpu.VMEM)


def on_device(
    histories, amplitude, weights, retarded, owner_block, owner_cell, adjoint, step_size, jacobian
):
    groups = lax.axis_size("obs")
    count = lax.axis_size("cells")
    panels = weights.shape[0]
    chunks = panels // TILE
    blocks2 = owner_block.reshape(chunks, TILE)
    cells2 = owner_cell.reshape(chunks, TILE)
    amp = amplitude.transpose(1, 0, 2)
    edge = pltpu.VMEM((COMP,) + adjoint.shape[2:], F32)

    partial_copies, head, tail = pl.pallas_call(
        project,
        out_shape=(pltpu.VMEM((groups, 56, TILE), F32), edge, edge),
        in_specs=[VMEM, VMEM, ANY, ANY, ANY],
        out_specs=(VMEM, VMEM, VMEM),
        scratch_shapes=[
            pltpu.VMEM(amp.shape, BF16),
            pltpu.VMEM(weights.shape, BF16),
            pltpu.VMEM(adjoint.shape, F32),
            pltpu.SemaphoreType.DMA((3,)),
        ],
        name="project",
    )(histories, retarded.T, amp, weights, adjoint)
    parts = lax.all_to_all(partial_copies, "obs", split_axis=0, concat_axis=0, tiled=True)
    behind = lax.ppermute(tail, "cells", [(i, (i + 1) % count) for i in range(count)])
    ahead = lax.ppermute(head, "cells", [((i + 1) % count, i) for i in range(count)])

    same, slot = pl.pallas_call(
        order,
        out_shape=(pltpu.VMEM((chunks, 128, TILE), BF16), pltpu.VMEM((chunks, CAP, TILE), BF16)),
        in_specs=[ANY, VMEM],
        out_specs=(VMEM, VMEM),
        name="order",
    )(partial_copies, blocks2)
    parts, ahead, behind = lax.optimization_barrier((parts, ahead, behind))
    panel_source, outgoing = pl.pallas_call(
        pack,
        out_shape=(jax.ShapeDtypeStruct((COMP, panels), F32), pltpu.VMEM((count, 256), F32)),
        in_specs=[VMEM] * 4,
        out_specs=(VMEM, VMEM),
        name="pack",
    )(near(parts), near(same), near(slot), cells2)
    received = lax.all_to_all(outgoing, "cells", split_axis=0, concat_axis=0, tiled=True)

    base = pl.pallas_call(
        stencil,
        out_shape=pltpu.VMEM(adjoint.shape, F32),
        in_specs=[VMEM] * 5 + [SMEM],
        out_specs=VMEM,
        name="stencil",
    )(near(parts), near(ahead), near(behind), adjoint, step_size, jacobian.transpose(1, 2, 0, 3))
    adjoint_next = pl.pallas_call(
        land,
        out_shape=jax.ShapeDtypeStruct(adjoint.shape, F32),
        in_specs=[VMEM] * 2,
        out_specs=VMEM,
        name="land",
    )(near(received), near(base))
    return adjoint_next, panel_source


def solution(mesh):
    return jax.shard_map(
        on_device,
        mesh=mesh,
        in_specs=(
            P("obs", None),
            P("obs", None, "cells"),
            P("cells", None),
            P("obs", "cells"),
            P("cells"),
            P("cells"),
            P(None, "cells", "obs", None),
            P("cells", "obs", None),
            P("cells", None, None, None),
        ),
        out_specs=(P(None, "cells", "obs", None), P(None, "cells")),
        check_vma=False,
    )
```

```python
import jax
import jax.numpy as jnp
from jax import lax
from jax.experimental import pallas as pl
from jax.experimental.pallas import tpu as pltpu
from jax.sharding import PartitionSpec as P


TILE = 128
COMP = 5
CAP = 32
SMOOTHING = 0.25
F32 = jnp.float32
BF16 = jnp.bfloat16
NT = (((1,), (1,)), ((), ()))

VMEM = pl.BlockSpec(memory_space=pltpu.MemorySpace.VMEM)
SMEM = pl.BlockSpec(memory_space=pltpu.MemorySpace.SMEM)
ANY = pl.BlockSpec(memory_space=pl.ANY)


def iota(shape, dim):
    return lax.broadcasted_iota(jnp.int32, shape, dim)


def project(hist_ref, ret_ref, amp_hbm, weight_hbm, adj_hbm, out_ref, head_ref, tail_ref, amp_ref, weight_ref, adj_ref, sems):
    moves = [
        pltpu.make_async_copy(source, target, sems.at[i])
        for i, (source, target) in enumerate(((weight_hbm, weight_ref), (amp_hbm, amp_ref), (adj_hbm, adj_ref)))
    ]
    for move in moves:
        move.start()
    group = lax.axis_index("obs")
    observers = hist_ref.shape[0]
    tiles = ret_ref.shape[0]
    hist = hist_ref[...].astype(F32)
    rows = tiles * observers
    column = [jnp.concatenate([hist[:, j * 128 : (j + 1) * 128]] * tiles, axis=0) for j in range(3)]
    eye = iota((observers, observers), 0) == iota((observers, observers), 1)
    shift = jnp.concatenate(
        [
            jnp.broadcast_to(
                jnp.sum(jnp.where(eye, ret_ref[t : t + 1, :].astype(F32), 0.0), axis=1, keepdims=True), (observers, 128)
            )
            for t in range(tiles)
        ],
        axis=0,
    ).astype(jnp.int32)
    lane = iota((rows, 128), 1)
    far = shift >= 128
    column = [
        jnp.where(far, column[1], column[0]),
        jnp.where(far, column[2], column[1]),
        column[2],
    ]
    for amount in (64, 32, 16, 8, 4, 2, 1):
        turned = [pltpu.roll(x, 128 - amount, 1) for x in column]
        stays = lane < 128 - amount
        chosen = (shift & amount) != 0
        column = [
            jnp.where(chosen, jnp.where(stays, turned[0], turned[1]), column[0]),
            jnp.where(chosen, jnp.where(stays, turned[1], turned[2]), column[1]),
            jnp.where(chosen, turned[2], column[2]),
        ]
    window = jnp.concatenate(column[:2], axis=1).astype(BF16)
    for move in moves:
        move.wait()
    copies = out_ref.shape[0]
    for t in range(tiles):
        span = slice(t * TILE, (t + 1) * TILE)
        projected = lax.dot_general(
            window[t * observers : (t + 1) * observers],
            weight_ref[span, :],
            NT,
            preferred_element_type=F32,
        )
        for c in range(COMP):
            total = jnp.sum(amp_ref[c, :, span].astype(F32) * projected, axis=0, keepdims=True)
            for copy in range(copies):
                out_ref[copy, c * tiles + t : c * tiles + t + 1, :] = total
    azimuths, radii = adj_ref.shape[1:3]
    head_ref[...] = adj_ref[:, 0]
    tail_ref[...] = adj_ref[:, azimuths - 1]
    for c in range(COMP):
        for a in range(azimuths):
            place = COMP * tiles + c * azimuths + a
            for copy in range(copies):
                up = jnp.full((1, 128), copy, jnp.int32) > group
                out_ref[copy, place : place + 1, :] = jnp.where(
                    up, adj_ref[c, a, radii - 1 : radii, :], adj_ref[c, a, 0:1, :]
                )
    for copy in range(copies):
        out_ref[copy, 50:56, :] = jnp.zeros((6, 128), F32)


def order(after_ref, block_ref, cell_ref, same_ref, slot_ref, line_ref):
    chunks, width = block_ref.shape
    blocks = 128
    mark = jnp.where((iota((width, 2 * width), 0) < iota((width, 2 * width), 1)), 1.0, 0.0).astype(BF16)
    line_ref[...] = cell_ref[...].astype(F32)
    before = jnp.zeros((blocks, width), F32)
    for j in range(chunks):
        same = iota((blocks, width), 0) == block_ref[j : j + 1, :]
        marked = jnp.where(same, 1.0, 0.0).astype(BF16)
        same_ref[j] = marked
        counted = jnp.dot(marked, mark, preferred_element_type=F32)
        rank = jnp.sum(jnp.where(same, counted[:, :width] + before, 0.0), axis=0, keepdims=True)
        slot_ref[j] = jnp.where(iota((CAP, width), 0).astype(F32) == rank, 1.0, 0.0).astype(BF16)
        before = before + counted[:, width:]


def whole_source(part_ref, count):
    source = part_ref[0, :count, :]
    for group in range(1, part_ref.shape[0]):
        source = source + part_ref[group, :count, :]
    return source


def pack(part_ref, same_ref, slot_ref, line_ref, out_ref):
    chunks, width = line_ref.shape
    lines = jnp.concatenate([whole_source(part_ref, COMP * chunks), line_ref[...]], axis=0)
    high = lines.astype(BF16).astype(F32)
    low = lines - high
    total = jnp.zeros((128, (COMP + 1) * CAP), F32)
    for j in range(chunks):
        slot = slot_ref[j]
        placed = []
        for part in (high, low):
            placed.append(
                jnp.concatenate(
                    [
                        jnp.broadcast_to(part[c * chunks + j : c * chunks + j + 1, :], (CAP, width)).astype(BF16) * slot
                        for c in range(COMP + 1)
                    ],
                    axis=0,
                )
            )
        same = same_ref[j]
        total = total + lax.dot_general(
            jnp.concatenate([same, same], axis=1),
            jnp.concatenate(placed, axis=1),
            NT,
            preferred_element_type=F32,
        )
    rest = jnp.concatenate([total[:, 128:], jnp.zeros((128, 64), F32)], axis=1)
    out_ref[:, 0, :] = jnp.concatenate([total[:, :128], rest], axis=1)


def stencil(part_ref, next_ref, prev_ref, adj_ref, step_ref, jac_ref, out_ref, source_ref):
    chunks = source_ref.shape[1] // TILE
    source = whole_source(part_ref, COMP * chunks)
    for c in range(COMP):
        for j in range(chunks):
            source_ref[c : c + 1, j * TILE : (j + 1) * TILE] = source[c * chunks + j : c * chunks + j + 1, :]
    group = lax.axis_index("obs")
    groups = part_ref.shape[0]
    azimuths, radii, length = adj_ref.shape[1:]
    row = iota((radii, length), 0)
    lane = iota((radii, length), 1)
    below = jnp.maximum(group - 1, 0)
    above = jnp.minimum(group + 1, groups - 1)
    has_below = jnp.where(group > 0, 1.0, 0.0)
    has_above = jnp.where(group < groups - 1, 1.0, 0.0)
    uppers = part_ref[above, 40:56, :] * has_above
    lowers = part_ref[below, 40:56, :] * has_below
    for a in range(azimuths):
        centre = [adj_ref[c, a] for c in range(COMP)]
        pairs = [[], [], []]
        for c in range(COMP):
            x = centre[c]
            ahead = next_ref[c] if a == azimuths - 1 else adj_ref[c, a + 1]
            behind = prev_ref[c] if a == 0 else adj_ref[c, a - 1]
            pairs[0].append((ahead, behind))
            place = c * azimuths + a
            upper = uppers[place : place + 1]
            lower = lowers[place : place + 1]
            pairs[1].append(
                (
                    jnp.where(row == radii - 1, upper, pltpu.roll(x, radii - 1, 0)),
                    jnp.where(row == 0, lower, pltpu.roll(x, 1, 0)),
                )
            )
            pairs[2].append(
                (
                    jnp.where(lane == length - 1, 0.0, pltpu.roll(x, length - 1, 1)),
                    jnp.where(lane == 0, 0.0, pltpu.roll(x, 1, 1)),
                )
            )
        differences = [[f - b for f, b in pairs[d]] for d in range(3)]
        for c in range(COMP):
            rotated = jnp.zeros((radii, length), F32)
            spread = -6.0 * centre[c]
            for d in range(3):
                spread = spread + (pairs[d][c][0] + pairs[d][c][1])
                for k in range(COMP):
                    rotated = rotated + jac_ref[d, k, 0, c] * differences[d][k]
            summed = 0.5 * rotated + SMOOTHING * spread
            out_ref[c, a] = centre[c] + step_ref[a] * summed


def land(got_ref, base_ref, out_ref):
    group = lax.axis_index("obs")
    azimuths, radii, length = base_ref.shape[1:]
    radii_all = radii * lax.axis_size("obs")
    local_rows = azimuths * radii
    got = jnp.concatenate([got_ref[:, :128].T, got_ref[:, 128:].T], axis=0)
    sources = got_ref.shape[0]
    high = got.astype(BF16).astype(F32)
    low = got - high
    cell = got[COMP * CAP : (COMP + 1) * CAP].astype(jnp.int32)
    cell_row = cell >> 7
    cell_lane = cell & 127
    local = iota((local_rows, sources), 0)
    wanted = (local // radii) * radii_all + local % radii + group * radii
    total = jnp.zeros((2 * COMP * local_rows, length), F32)
    for first in range(0, CAP, 2):
        values, lanes = [], []
        for k in (first, first + 1):
            here = jnp.where(wanted == cell_row[k : k + 1], 1.0, 0.0).astype(BF16)
            values.append(
                jnp.concatenate(
                    [
                        jnp.broadcast_to(part[c * CAP + k : c * CAP + k + 1], (local_rows, sources)).astype(BF16) * here
                        for part in (high, low)
                        for c in range(COMP)
                    ],
                    axis=0,
                )
            )
            lanes.append(jnp.where(iota((length, sources), 0) == cell_lane[k : k + 1], 1.0, 0.0).astype(BF16))
        total = total + lax.dot_general(
            jnp.concatenate(values, axis=1), jnp.concatenate(lanes, axis=1), NT, preferred_element_type=F32
        )
    half = COMP * local_rows
    for c in range(COMP):
        for a in range(azimuths):
            start = (c * azimuths + a) * radii
            out_ref[c, a] = base_ref[c, a] + (total[start : start + radii] + total[half + start : half + start + radii])


def near(x):
    return pltpu.with_memory_space_constraint(x, pltpu.VMEM)


def on_device(
    histories, amplitude, weights, retarded, owner_block, owner_cell, adjoint, step_size, jacobian
):
    groups = lax.axis_size("obs")
    count = lax.axis_size("cells")
    panels = weights.shape[0]
    chunks = panels // TILE
    blocks2 = owner_block.reshape(chunks, TILE)
    cells2 = owner_cell.reshape(chunks, TILE)
    amp = amplitude.transpose(1, 0, 2)
    edge = pltpu.VMEM((COMP,) + adjoint.shape[2:], F32)

    partial_copies, head, tail = pl.pallas_call(
        project,
        out_shape=(pltpu.VMEM((groups, 56, TILE), F32), edge, edge),
        in_specs=[VMEM, VMEM, ANY, ANY, ANY],
        out_specs=(VMEM, VMEM, VMEM),
        scratch_shapes=[
            pltpu.VMEM(amp.shape, BF16),
            pltpu.VMEM(weights.shape, BF16),
            pltpu.VMEM(adjoint.shape, F32),
            pltpu.SemaphoreType.DMA((3,)),
        ],
        name="project",
    )(histories, retarded.T, amp, weights, adjoint)
    parts = lax.all_to_all(partial_copies, "obs", split_axis=0, concat_axis=0, tiled=True)
    behind = lax.ppermute(tail, "cells", [(i, (i + 1) % count) for i in range(count)])
    ahead = lax.ppermute(head, "cells", [((i + 1) % count, i) for i in range(count)])

    same, slot, lines = pl.pallas_call(
        order,
        out_shape=(
            pltpu.VMEM((chunks, 128, TILE), BF16),
            pltpu.VMEM((chunks, CAP, TILE), BF16),
            pltpu.VMEM((chunks, TILE), F32),
        ),
        in_specs=[ANY, VMEM, VMEM],
        out_specs=(VMEM, VMEM, VMEM),
        name="order",
    )(partial_copies, blocks2, cells2)
    outgoing = pl.pallas_call(
        pack,
        out_shape=jax.ShapeDtypeStruct((count, 1, 256), F32),
        in_specs=[VMEM] * 4,
        out_specs=VMEM,
        name="pack",
    )(near(parts), near(same), near(slot), near(lines))
    received = lax.all_to_all(outgoing, "cells", split_axis=0, concat_axis=0, tiled=True)

    base, panel_source = pl.pallas_call(
        stencil,
        out_shape=(pltpu.VMEM(adjoint.shape, F32), jax.ShapeDtypeStruct((COMP, panels), F32)),
        in_specs=[VMEM] * 5 + [SMEM],
        out_specs=(VMEM, VMEM),
        name="stencil",
    )(near(parts), near(ahead), near(behind), adjoint, step_size, jacobian.transpose(1, 2, 0, 3))
    adjoint_next = pl.pallas_call(
        land,
        out_shape=jax.ShapeDtypeStruct(adjoint.shape, F32),
        in_specs=[VMEM] * 2,
        out_specs=VMEM,
        name="land",
    )(near(received.reshape(count, 256)), near(base))
    return adjoint_next, panel_source


def solution(mesh):
    return jax.shard_map(
        on_device,
        mesh=mesh,
        in_specs=(
            P("obs", None),
            P("obs", None, "cells"),
            P("cells", None),
            P("obs", "cells"),
            P("cells"),
            P("cells"),
            P(None, "cells", "obs", None),
            P("cells", "obs", None),
            P("cells", None, None, None),
        ),
        out_specs=(P(None, "cells", "obs", None), P(None, "cells")),
        check_vma=False,
    )
```

```python
import jax
import jax.numpy as jnp
from jax import lax
from jax.experimental import pallas as pl
from jax.experimental.pallas import tpu as pltpu
from jax.sharding import PartitionSpec as P


TILE = 128
COMP = 5
CAP = 32
SMOOTHING = 0.25
F32 = jnp.float32
BF16 = jnp.bfloat16
NT = (((1,), (1,)), ((), ()))
FIRST_CELL = 75
FIRST_GROUP = 0

VMEM = pl.BlockSpec(memory_space=pltpu.MemorySpace.VMEM)
SMEM = pl.BlockSpec(memory_space=pltpu.MemorySpace.SMEM)
ANY = pl.BlockSpec(memory_space=pl.ANY)


def iota(shape, dim):
    return lax.broadcasted_iota(jnp.int32, shape, dim)


def project(hist_ref, ret_ref, amp_hbm, weight_hbm, adj_hbm, out_ref, head_ref, tail_ref, amp_ref, weight_ref, adj_ref, sems):
    moves = [
        pltpu.make_async_copy(source, target, sems.at[i])
        for i, (source, target) in enumerate(((weight_hbm, weight_ref), (amp_hbm, amp_ref), (adj_hbm, adj_ref)))
    ]
    for move in moves:
        move.start()
    group = lax.axis_index("obs")
    observers = hist_ref.shape[0]
    tiles = ret_ref.shape[0]
    hist = hist_ref[...].astype(F32)
    rows = tiles * observers
    column = [jnp.concatenate([hist[:, j * 128 : (j + 1) * 128]] * tiles, axis=0) for j in range(3)]
    eye = iota((observers, observers), 0) == iota((observers, observers), 1)
    shift = jnp.concatenate(
        [
            jnp.broadcast_to(
                jnp.sum(jnp.where(eye, ret_ref[t : t + 1, :].astype(F32), 0.0), axis=1, keepdims=True), (observers, 128)
            )
            for t in range(tiles)
        ],
        axis=0,
    ).astype(jnp.int32)
    lane = iota((rows, 128), 1)
    far = shift >= 128
    column = [
        jnp.where(far, column[1], column[0]),
        jnp.where(far, column[2], column[1]),
        column[2],
    ]
    for amount in (64, 32, 16, 8, 4, 2, 1):
        turned = [pltpu.roll(x, 128 - amount, 1) for x in column]
        stays = lane < 128 - amount
        chosen = (shift & amount) != 0
        column = [
            jnp.where(chosen, jnp.where(stays, turned[0], turned[1]), column[0]),
            jnp.where(chosen, jnp.where(stays, turned[1], turned[2]), column[1]),
            jnp.where(chosen, turned[2], column[2]),
        ]
    window = jnp.concatenate(column[:2], axis=1).astype(BF16)
    for move in moves:
        move.wait()
    copies = out_ref.shape[0]
    for t in range(tiles):
        span = slice(t * TILE, (t + 1) * TILE)
        projected = lax.dot_general(
            window[t * observers : (t + 1) * observers],
            weight_ref[span, :],
            NT,
            preferred_element_type=F32,
        )
        for c in range(COMP):
            total = jnp.sum(amp_ref[c, :, span].astype(F32) * projected, axis=0, keepdims=True)
            for copy in range(copies):
                out_ref[copy, c * tiles + t : c * tiles + t + 1, :] = total
    azimuths, radii = adj_ref.shape[1:3]
    head_ref[...] = adj_ref[:, 0]
    tail_ref[...] = adj_ref[:, azimuths - 1]
    for c in range(COMP):
        for a in range(azimuths):
            place = COMP * tiles + c * azimuths + a
            for copy in range(copies):
                up = jnp.full((1, 128), (copy + FIRST_GROUP) % copies, jnp.int32) > group
                out_ref[copy, place : place + 1, :] = jnp.where(
                    up, adj_ref[c, a, radii - 1 : radii, :], adj_ref[c, a, 0:1, :]
                )
    for copy in range(copies):
        out_ref[copy, 50:56, :] = jnp.zeros((6, 128), F32)


def order(after_ref, block_ref, cell_ref, same_ref, slot_ref, line_ref):
    chunks, width = block_ref.shape
    blocks = 128
    mark = jnp.where((iota((width, 2 * width), 0) < iota((width, 2 * width), 1)), 1.0, 0.0).astype(BF16)
    line_ref[...] = cell_ref[...].astype(F32)
    named = (iota((blocks, width), 0) + FIRST_CELL) % blocks
    before = jnp.zeros((blocks, width), F32)
    for j in range(chunks):
        same = named == block_ref[j : j + 1, :]
        marked = jnp.where(same, 1.0, 0.0).astype(BF16)
        same_ref[j] = marked
        counted = jnp.dot(marked, mark, preferred_element_type=F32)
        rank = jnp.sum(jnp.where(same, counted[:, :width] + before, 0.0), axis=0, keepdims=True)
        slot_ref[j] = jnp.where(iota((CAP, width), 0).astype(F32) == rank, 1.0, 0.0).astype(BF16)
        before = before + counted[:, width:]


def whole_source(part_ref, count):
    source = part_ref[0, :count, :]
    for group in range(1, part_ref.shape[0]):
        source = source + part_ref[group, :count, :]
    return source


def pack(part_ref, same_ref, slot_ref, line_ref, out_ref):
    chunks, width = line_ref.shape
    lines = jnp.concatenate([whole_source(part_ref, COMP * chunks), line_ref[...]], axis=0)
    high = lines.astype(BF16).astype(F32)
    low = lines - high
    total = jnp.zeros((128, (COMP + 1) * CAP), F32)
    for j in range(chunks):
        slot = slot_ref[j]
        placed = []
        for part in (high, low):
            placed.append(
                jnp.concatenate(
                    [
                        jnp.broadcast_to(part[c * chunks + j : c * chunks + j + 1, :], (CAP, width)).astype(BF16) * slot
                        for c in range(COMP + 1)
                    ],
                    axis=0,
                )
            )
        same = same_ref[j]
        total = total + lax.dot_general(
            jnp.concatenate([same, same], axis=1),
            jnp.concatenate(placed, axis=1),
            NT,
            preferred_element_type=F32,
        )
    rest = jnp.concatenate([total[:, 128:], jnp.zeros((128, 64), F32)], axis=1)
    out_ref[:, 0, :] = jnp.concatenate([total[:, :128], rest], axis=1)


def stencil(part_ref, next_ref, prev_ref, adj_ref, step_ref, jac_ref, out_ref, source_ref):
    chunks = source_ref.shape[1] // TILE
    source = whole_source(part_ref, COMP * chunks)
    for c in range(COMP):
        for j in range(chunks):
            source_ref[c : c + 1, j * TILE : (j + 1) * TILE] = source[c * chunks + j : c * chunks + j + 1, :]
    group = lax.axis_index("obs")
    groups = part_ref.shape[0]
    azimuths, radii, length = adj_ref.shape[1:]
    row = iota((radii, length), 0)
    lane = iota((radii, length), 1)
    below = jnp.maximum(group - 1, 0)
    above = jnp.minimum(group + 1, groups - 1)
    has_below = jnp.where(group > 0, 1.0, 0.0)
    has_above = jnp.where(group < groups - 1, 1.0, 0.0)
    uppers = part_ref[(above - FIRST_GROUP + groups) % groups, 40:56, :] * has_above
    lowers = part_ref[(below - FIRST_GROUP + groups) % groups, 40:56, :] * has_below
    for a in range(azimuths):
        centre = [adj_ref[c, a] for c in range(COMP)]
        pairs = [[], [], []]
        for c in range(COMP):
            x = centre[c]
            ahead = next_ref[c] if a == azimuths - 1 else adj_ref[c, a + 1]
            behind = prev_ref[c] if a == 0 else adj_ref[c, a - 1]
            pairs[0].append((ahead, behind))
            place = c * azimuths + a
            upper = uppers[place : place + 1]
            lower = lowers[place : place + 1]
            pairs[1].append(
                (
                    jnp.where(row == radii - 1, upper, pltpu.roll(x, radii - 1, 0)),
                    jnp.where(row == 0, lower, pltpu.roll(x, 1, 0)),
                )
            )
            pairs[2].append(
                (
                    jnp.where(lane == length - 1, 0.0, pltpu.roll(x, length - 1, 1)),
                    jnp.where(lane == 0, 0.0, pltpu.roll(x, 1, 1)),
                )
            )
        differences = [[f - b for f, b in pairs[d]] for d in range(3)]
        for c in range(COMP):
            rotated = jnp.zeros((radii, length), F32)
            spread = -6.0 * centre[c]
            for d in range(3):
                spread = spread + (pairs[d][c][0] + pairs[d][c][1])
                for k in range(COMP):
                    rotated = rotated + jac_ref[d, k, 0, c] * differences[d][k]
            summed = 0.5 * rotated + SMOOTHING * spread
            out_ref[c, a] = centre[c] + step_ref[a] * summed


def land(got_ref, base_ref, out_ref):
    group = lax.axis_index("obs")
    azimuths, radii, length = base_ref.shape[1:]
    radii_all = radii * lax.axis_size("obs")
    local_rows = azimuths * radii
    got = jnp.concatenate([got_ref[:, :128].T, got_ref[:, 128:].T], axis=0)
    sources = got_ref.shape[0]
    high = got.astype(BF16).astype(F32)
    low = got - high
    cell = got[COMP * CAP : (COMP + 1) * CAP].astype(jnp.int32)
    cell_row = cell >> 7
    cell_lane = cell & 127
    local = iota((local_rows, sources), 0)
    wanted = (local // radii) * radii_all + local % radii + group * radii
    total = jnp.zeros((2 * COMP * local_rows, length), F32)
    for first in range(0, CAP, 2):
        values, lanes = [], []
        for k in (first, first + 1):
            here = jnp.where(wanted == cell_row[k : k + 1], 1.0, 0.0).astype(BF16)
            values.append(
                jnp.concatenate(
                    [
                        jnp.broadcast_to(part[c * CAP + k : c * CAP + k + 1], (local_rows, sources)).astype(BF16) * here
                        for part in (high, low)
                        for c in range(COMP)
                    ],
                    axis=0,
                )
            )
            lanes.append(jnp.where(iota((length, sources), 0) == cell_lane[k : k + 1], 1.0, 0.0).astype(BF16))
        total = total + lax.dot_general(
            jnp.concatenate(values, axis=1), jnp.concatenate(lanes, axis=1), NT, preferred_element_type=F32
        )
    half = COMP * local_rows
    for c in range(COMP):
        for a in range(azimuths):
            start = (c * azimuths + a) * radii
            out_ref[c, a] = base_ref[c, a] + (total[start : start + radii] + total[half + start : half + start + radii])


def turned(size, first):
    return [[(i + first) % size for i in range(size)]]


def near(x):
    return pltpu.with_memory_space_constraint(x, pltpu.VMEM)


def on_device(
    histories, amplitude, weights, retarded, owner_block, owner_cell, adjoint, step_size, jacobian
):
    groups = lax.axis_size("obs")
    count = lax.axis_size("cells")
    panels = weights.shape[0]
    chunks = panels // TILE
    blocks2 = owner_block.reshape(chunks, TILE)
    cells2 = owner_cell.reshape(chunks, TILE)
    amp = amplitude.transpose(1, 0, 2)
    edge = pltpu.VMEM((COMP,) + adjoint.shape[2:], F32)

    partial_copies, head, tail = pl.pallas_call(
        project,
        out_shape=(pltpu.VMEM((groups, 56, TILE), F32), edge, edge),
        in_specs=[VMEM, VMEM, ANY, ANY, ANY],
        out_specs=(VMEM, VMEM, VMEM),
        scratch_shapes=[
            pltpu.VMEM(amp.shape, BF16),
            pltpu.VMEM(weights.shape, BF16),
            pltpu.VMEM(adjoint.shape, F32),
            pltpu.SemaphoreType.DMA((3,)),
        ],
        name="project",
    )(histories, retarded.T, amp, weights, adjoint)
    parts = lax.all_to_all(
        partial_copies, "obs", 0, 0, axis_index_groups=turned(groups, FIRST_GROUP), tiled=True
    )
    behind = lax.ppermute(tail, "cells", [(i, (i + 1) % count) for i in range(count)])
    ahead = lax.ppermute(head, "cells", [((i + 1) % count, i) for i in range(count)])

    same, slot, lines = pl.pallas_call(
        order,
        out_shape=(
            pltpu.VMEM((chunks, 128, TILE), BF16),
            pltpu.VMEM((chunks, CAP, TILE), BF16),
            pltpu.VMEM((chunks, TILE), F32),
        ),
        in_specs=[ANY, VMEM, VMEM],
        out_specs=(VMEM, VMEM, VMEM),
        name="order",
    )(partial_copies, blocks2, cells2)
    outgoing = pl.pallas_call(
        pack,
        out_shape=jax.ShapeDtypeStruct((count, 1, 256), F32),
        in_specs=[VMEM] * 4,
        out_specs=VMEM,
        name="pack",
    )(near(parts), near(same), near(slot), near(lines))
    received = lax.all_to_all(
        outgoing, "cells", 0, 0, axis_index_groups=turned(count, FIRST_CELL), tiled=True
    )

    base, panel_source = pl.pallas_call(
        stencil,
        out_shape=(pltpu.VMEM(adjoint.shape, F32), jax.ShapeDtypeStruct((COMP, panels), F32)),
        in_specs=[VMEM] * 5 + [SMEM],
        out_specs=(VMEM, VMEM),
        name="stencil",
    )(near(parts), near(ahead), near(behind), adjoint, step_size, jacobian.transpose(1, 2, 0, 3))
    adjoint_next = pl.pallas_call(
        land,
        out_shape=jax.ShapeDtypeStruct(adjoint.shape, F32),
        in_specs=[VMEM] * 2,
        out_specs=VMEM,
        name="land",
    )(near(received.reshape(count, 256)), near(base))
    return adjoint_next, panel_source


def solution(mesh):
    return jax.shard_map(
        on_device,
        mesh=mesh,
        in_specs=(
            P("obs", None),
            P("obs", None, "cells"),
            P("cells", None),
            P("obs", "cells"),
            P("cells"),
            P("cells"),
            P(None, "cells", "obs", None),
            P("cells", "obs", None),
            P("cells", None, None, None),
        ),
        out_specs=(P(None, "cells", "obs", None), P(None, "cells")),
        check_vma=False,
    )
```

```python
import jax
import jax.numpy as jnp
from jax import lax
from jax.experimental import pallas as pl
from jax.experimental.pallas import tpu as pltpu
from jax.sharding import PartitionSpec as P


TILE = 128
COMP = 5
CAP = 32
SMOOTHING = 0.25
F32 = jnp.float32
BF16 = jnp.bfloat16
NT = (((1,), (1,)), ((), ()))
FIRST_CELL = 75
FIRST_GROUP = 2

VMEM = pl.BlockSpec(memory_space=pltpu.MemorySpace.VMEM)
SMEM = pl.BlockSpec(memory_space=pltpu.MemorySpace.SMEM)
ANY = pl.BlockSpec(memory_space=pl.ANY)


def iota(shape, dim):
    return lax.broadcasted_iota(jnp.int32, shape, dim)


def project(
    hist_hbm, ret_hbm, adj_hbm, weight_hbm, amp_hbm, block_hbm, cell_hbm, step_hbm,
    out_hbm, inner_ref, outer_ref, adj_ref, block_ref, cell_ref, step_ref,
    hist_ref, ret_ref, weight_ref, amp_ref, part_ref, line_ref, sems,
):
    group = lax.axis_index("obs")
    odd = lax.axis_index("cells") % 2
    copies = out_hbm.shape[0]
    tiles, observers = ret_hbm.shape
    azimuths, radii = adj_ref.shape[1:3]
    count = COMP * tiles
    half = tiles * TILE // 2
    moves = [
        pltpu.make_async_copy(source, target, sems.at[i])
        for i, (source, target) in enumerate(
            (
                (hist_hbm, hist_ref),
                (ret_hbm, ret_ref),
                (adj_hbm, adj_ref),
                (weight_hbm.at[:half], weight_ref.at[:half]),
                (amp_hbm.at[:, :, :half], amp_ref.at[:, :, :half]),
                (weight_hbm.at[half:], weight_ref.at[half:]),
                (amp_hbm.at[:, :, half:], amp_ref.at[:, :, half:]),
                (block_hbm, block_ref),
                (cell_hbm, cell_ref),
                (step_hbm, step_ref),
            )
        )
    ]
    for move in moves:
        move.start()
    moves[0].wait()
    moves[1].wait()
    hist = hist_ref[...].astype(F32)
    rows = tiles * observers
    column = [jnp.concatenate([hist[:, j * 128 : (j + 1) * 128]] * tiles, axis=0) for j in range(3)]
    eye = iota((observers, observers), 0) == iota((observers, observers), 1)
    shift = jnp.concatenate(
        [
            jnp.broadcast_to(
                jnp.sum(jnp.where(eye, ret_ref[t : t + 1, :].astype(F32), 0.0), axis=1, keepdims=True), (observers, 128)
            )
            for t in range(tiles)
        ],
        axis=0,
    ).astype(jnp.int32)
    lane = iota((rows, 128), 1)
    far = shift >= 128
    column = [
        jnp.where(far, column[1], column[0]),
        jnp.where(far, column[2], column[1]),
        column[2],
    ]
    for amount in (64, 32, 16, 8, 4, 2, 1):
        rolled = [pltpu.roll(x, 128 - amount, 1) for x in column]
        stays = lane < 128 - amount
        chosen = (shift & amount) != 0
        column = [
            jnp.where(chosen, jnp.where(stays, rolled[0], rolled[1]), column[0]),
            jnp.where(chosen, jnp.where(stays, rolled[1], rolled[2]), column[1]),
            jnp.where(chosen, rolled[2], column[2]),
        ]
    window = jnp.concatenate(column[:2], axis=1).astype(BF16)
    moves[2].wait()
    for upper, row in ((0, 0), (1, radii - 1)):
        for c in range(COMP):
            for a in range(azimuths):
                place = c * azimuths + a
                line_ref[upper, place : place + 1, :] = adj_ref[c, a, row : row + 1, :]
        line_ref[upper, 10:16, :] = jnp.zeros((6, 128), F32)
    sends = []
    for copy in range(copies):
        upper = jnp.where((copy + FIRST_GROUP) % copies > group, 1, 0)
        sends.append(
            pltpu.make_async_copy(line_ref.at[upper], out_hbm.at[copy, pl.ds(count, 16)], sems.at[10 + copy])
        )
        sends[-1].start()
    even = odd == 0
    inner_ref[...] = jnp.where(even, adj_ref[:, azimuths - 1], adj_ref[:, 0])
    outer_ref[...] = jnp.where(even, adj_ref[:, 0], adj_ref[:, azimuths - 1])
    for t in range(tiles):
        if t == 0:
            moves[3].wait()
            moves[4].wait()
        if t == tiles // 2:
            moves[5].wait()
            moves[6].wait()
        span = slice(t * TILE, (t + 1) * TILE)
        projected = lax.dot_general(
            window[t * observers : (t + 1) * observers],
            weight_ref[span, :],
            NT,
            preferred_element_type=F32,
        )
        for c in range(COMP):
            part_ref[c * tiles + t : c * tiles + t + 1, :] = jnp.sum(
                amp_ref[c, :, span].astype(F32) * projected, axis=0, keepdims=True
            )
    for copy in range(copies):
        sends.append(
            pltpu.make_async_copy(part_ref, out_hbm.at[copy, pl.ds(0, count)], sems.at[10 + copies + copy])
        )
        sends[-1].start()
    for move in moves[7:] + sends:
        move.wait()


def order(after_ref, block_ref, cell_ref, same_ref, slot_ref, line_ref):
    chunks, width = block_ref.shape
    blocks = 128
    mark = jnp.where((iota((width, 2 * width), 0) < iota((width, 2 * width), 1)), 1.0, 0.0).astype(BF16)
    line_ref[...] = cell_ref[...].astype(F32)
    named = (iota((blocks, width), 0) + FIRST_CELL) % blocks
    before = jnp.zeros((blocks, width), F32)
    for j in range(chunks):
        same = named == block_ref[j : j + 1, :]
        marked = jnp.where(same, 1.0, 0.0).astype(BF16)
        same_ref[j] = marked
        counted = jnp.dot(marked, mark, preferred_element_type=F32)
        rank = jnp.sum(jnp.where(same, counted[:, :width] + before, 0.0), axis=0, keepdims=True)
        slot_ref[j] = jnp.where(iota((CAP, width), 0).astype(F32) == rank, 1.0, 0.0).astype(BF16)
        before = before + counted[:, width:]


def whole_source(part_ref, count):
    source = part_ref[0, :count, :]
    for group in range(1, part_ref.shape[0]):
        source = source + part_ref[group, :count, :]
    return source


def pack(part_ref, same_ref, slot_ref, line_ref, out_ref):
    chunks, width = line_ref.shape
    lines = jnp.concatenate([whole_source(part_ref, COMP * chunks), line_ref[...]], axis=0)
    high = lines.astype(BF16).astype(F32)
    low = lines - high
    total = jnp.zeros((128, (COMP + 1) * CAP), F32)
    for j in range(chunks):
        slot = slot_ref[j]
        placed = []
        for part in (high, low):
            placed.append(
                jnp.concatenate(
                    [
                        jnp.broadcast_to(part[c * chunks + j : c * chunks + j + 1, :], (CAP, width)).astype(BF16) * slot
                        for c in range(COMP + 1)
                    ],
                    axis=0,
                )
            )
        same = same_ref[j]
        total = total + lax.dot_general(
            jnp.concatenate([same, same], axis=1),
            jnp.concatenate(placed, axis=1),
            NT,
            preferred_element_type=F32,
        )
    rest = jnp.concatenate([total[:, 128:], jnp.zeros((128, 64), F32)], axis=1)
    out_ref[:, 0, :] = jnp.concatenate([total[:, :128], rest], axis=1)


def stencil(part_ref, inner_ref, adj_ref, step_ref, jac_ref, out_ref, source_ref, mix_ref):
    chunks = source_ref.shape[1] // TILE
    source = whole_source(part_ref, COMP * chunks)
    for c in range(COMP):
        for j in range(chunks):
            source_ref[c : c + 1, j * TILE : (j + 1) * TILE] = source[c * chunks + j : c * chunks + j + 1, :]
    group = lax.axis_index("obs")
    groups = part_ref.shape[0]
    azimuths, radii, length = adj_ref.shape[1:]
    row = iota((radii, length), 0)
    lane = iota((radii, length), 1)
    below = jnp.maximum(group - 1, 0)
    above = jnp.minimum(group + 1, groups - 1)
    has_below = jnp.where(group > 0, 1.0, 0.0)
    has_above = jnp.where(group < groups - 1, 1.0, 0.0)
    even = lax.axis_index("cells") % 2 == 0
    half = jnp.where(even, -0.5, 0.5)
    for k in range(COMP):
        for c in range(COMP):
            weight = jac_ref[0, k, 0, c] * half + (SMOOTHING if k == c else 0.0)
            mix_ref[k * COMP + c : k * COMP + c + 1, :] = jnp.full((1, length), weight, F32)
    uppers = part_ref[(above - FIRST_GROUP + groups) % groups, 40:56, :] * has_above
    lowers = part_ref[(below - FIRST_GROUP + groups) % groups, 40:56, :] * has_below
    for a in range(azimuths):
        centre = [adj_ref[c, a] for c in range(COMP)]
        pairs = [[], [], []]
        for c in range(COMP):
            x = centre[c]
            ahead = jnp.where(even, inner_ref[c], 0.0) if a == azimuths - 1 else adj_ref[c, a + 1]
            behind = jnp.where(even, 0.0, inner_ref[c]) if a == 0 else adj_ref[c, a - 1]
            pairs[0].append((ahead, behind))
            place = c * azimuths + a
            upper = uppers[place : place + 1]
            lower = lowers[place : place + 1]
            pairs[1].append(
                (
                    jnp.where(row == radii - 1, upper, pltpu.roll(x, radii - 1, 0)),
                    jnp.where(row == 0, lower, pltpu.roll(x, 1, 0)),
                )
            )
            pairs[2].append(
                (
                    jnp.where(lane == length - 1, 0.0, pltpu.roll(x, length - 1, 1)),
                    jnp.where(lane == 0, 0.0, pltpu.roll(x, 1, 1)),
                )
            )
        differences = [[f - b for f, b in pairs[d]] for d in range(3)]
        for c in range(COMP):
            rotated = jnp.zeros((radii, length), F32)
            spread = -6.0 * centre[c]
            for d in range(3):
                spread = spread + (pairs[d][c][0] + pairs[d][c][1])
                for k in range(COMP):
                    rotated = rotated + jac_ref[d, k, 0, c] * differences[d][k]
            summed = 0.5 * rotated + SMOOTHING * spread
            out_ref[c, a] = centre[c] + step_ref[a] * summed


def land(got_ref, base_ref, outer_ref, step_ref, mix_ref, source_ref, out_ref, source_hbm, sem):
    move = pltpu.make_async_copy(source_ref, source_hbm, sem)
    move.start()
    group = lax.axis_index("obs")
    azimuths, radii, length = base_ref.shape[1:]
    radii_all = radii * lax.axis_size("obs")
    got = jnp.concatenate([got_ref[:, :128].T, got_ref[:, 128:].T], axis=0)
    sources = got_ref.shape[0]
    high = got.astype(BF16).astype(F32)
    low = got - high
    cell = got[COMP * CAP : (COMP + 1) * CAP].astype(jnp.int32)
    cell_row = (cell // length % radii_all).astype(F32)
    cell_column = (cell // (length * radii_all) * length + cell % length).astype(F32)
    wanted = (iota((radii, sources), 0) + group * radii).astype(F32).astype(BF16)
    columns = azimuths * length
    column = iota((columns, sources), 0).astype(F32).astype(BF16)
    one, none = jnp.ones((), BF16), jnp.zeros((), BF16)
    total = jnp.zeros((2 * COMP * radii, columns), F32)
    for first in range(0, CAP, 2):
        values, places = [], []
        for k in range(first, first + 2):
            row = jnp.broadcast_to(cell_row[k : k + 1], wanted.shape).astype(BF16)
            here = jnp.where(wanted == row, one, none)
            values.append(
                jnp.concatenate(
                    [
                        jnp.broadcast_to(part[c * CAP + k : c * CAP + k + 1], wanted.shape).astype(BF16) * here
                        for part in (high, low)
                        for c in range(COMP)
                    ],
                    axis=0,
                )
            )
            at = jnp.broadcast_to(cell_column[k : k + 1], column.shape).astype(BF16)
            places.append(jnp.where(column == at, one, none))
        total = total + lax.dot_general(
            jnp.concatenate(values, axis=1), jnp.concatenate(places, axis=1), NT, preferred_element_type=F32
        )
    half = COMP * radii
    edge = jnp.where(lax.axis_index("cells") % 2 == 0, 0, azimuths - 1)
    steps = [jnp.where(edge == a, step_ref[a], 0.0) for a in range(azimuths)]
    for c in range(COMP):
        spill = jnp.zeros((radii, length), F32)
        for k in range(COMP):
            spill = spill + mix_ref[k * COMP + c : k * COMP + c + 1, :] * outer_ref[k]
        for a in range(azimuths):
            rows = slice(c * radii, (c + 1) * radii)
            lower = slice(half + c * radii, half + (c + 1) * radii)
            span = slice(a * length, (a + 1) * length)
            out_ref[c, a] = base_ref[c, a] + steps[a] * spill + (total[rows, span] + total[lower, span])
    move.wait()


def turned(size, first):
    return [[(i + first) % size for i in range(size)]]


def near(x):
    return pltpu.with_memory_space_constraint(x, pltpu.VMEM)


def on_device(
    histories, amplitude, weights, retarded, owner_block, owner_cell, adjoint, step_size, jacobian
):
    groups = lax.axis_size("obs")
    count = lax.axis_size("cells")
    panels = weights.shape[0]
    chunks = panels // TILE
    blocks2 = owner_block.reshape(chunks, TILE)
    cells2 = owner_cell.reshape(chunks, TILE)
    amp = amplitude.transpose(1, 0, 2)
    edge = pltpu.VMEM((COMP,) + adjoint.shape[2:], F32)

    partial_copies, inner, outer, adjoint_near, blocks_near, cells_near, step_near = pl.pallas_call(
        project,
        out_shape=(
            jax.ShapeDtypeStruct((groups, 56, TILE), F32),
            edge,
            edge,
            pltpu.VMEM(adjoint.shape, F32),
            pltpu.VMEM(blocks2.shape, jnp.int32),
            pltpu.VMEM(cells2.shape, jnp.int32),
            pltpu.VMEM(step_size.shape, F32),
        ),
        in_specs=[ANY] * 8,
        out_specs=(ANY,) + (VMEM,) * 6,
        scratch_shapes=[
            pltpu.VMEM(histories.shape, BF16),
            pltpu.VMEM((chunks, histories.shape[0]), jnp.int32),
            pltpu.VMEM(weights.shape, BF16),
            pltpu.VMEM(amp.shape, BF16),
            pltpu.VMEM((COMP * chunks, TILE), F32),
            pltpu.VMEM((2, 16, TILE), F32),
            pltpu.SemaphoreType.DMA((10 + 2 * groups,)),
        ],
        name="project",
    )(histories, retarded.T, adjoint, weights, amp, blocks2, cells2, step_size)
    parts = lax.all_to_all(
        partial_copies, "obs", 0, 0, axis_index_groups=turned(groups, FIRST_GROUP), tiled=True
    )
    inner = lax.ppermute(inner, "cells", [(i, i ^ 1) for i in range(count)])
    outer = lax.ppermute(outer, "cells", [(i, ((i + 1 ^ 1) - 1) % count) for i in range(count)])

    same, slot, lines = pl.pallas_call(
        order,
        out_shape=(
            pltpu.VMEM((chunks, 128, TILE), BF16),
            pltpu.VMEM((chunks, CAP, TILE), BF16),
            pltpu.VMEM((chunks, TILE), F32),
        ),
        in_specs=[ANY, VMEM, VMEM],
        out_specs=(VMEM, VMEM, VMEM),
        name="order",
    )(partial_copies, near(blocks_near), near(cells_near))
    outgoing = pl.pallas_call(
        pack,
        out_shape=jax.ShapeDtypeStruct((count, 1, 256), F32),
        in_specs=[VMEM] * 4,
        out_specs=VMEM,
        name="pack",
    )(near(parts), near(same), near(slot), near(lines))
    received = lax.all_to_all(
        outgoing, "cells", 0, 0, axis_index_groups=turned(count, FIRST_CELL), tiled=True
    )

    base, source, mix = pl.pallas_call(
        stencil,
        out_shape=(
            pltpu.VMEM(adjoint.shape, F32),
            pltpu.VMEM((COMP, panels), F32),
            pltpu.VMEM((32, adjoint.shape[3]), F32),
        ),
        in_specs=[VMEM] * 4 + [SMEM],
        out_specs=(VMEM, VMEM, VMEM),
        name="stencil",
    )(near(parts), near(inner), near(adjoint_near), near(step_near), jacobian.transpose(1, 2, 0, 3))
    adjoint_next, panel_source = pl.pallas_call(
        land,
        out_shape=(
            jax.ShapeDtypeStruct(adjoint.shape, F32),
            jax.ShapeDtypeStruct((COMP, panels), F32),
        ),
        in_specs=[VMEM] * 6,
        out_specs=(VMEM, ANY),
        scratch_shapes=[pltpu.SemaphoreType.DMA],
        name="land",
    )(near(received.reshape(count, 256)), near(base), near(outer), near(step_near), near(mix), near(source))
    return adjoint_next, panel_source


def solution(mesh):
    return jax.shard_map(
        on_device,
        mesh=mesh,
        in_specs=(
            P("obs", None),
            P("obs", None, "cells"),
            P("cells", None),
            P("obs", "cells"),
            P("cells"),
            P("cells"),
            P(None, "cells", "obs", None),
            P("cells", "obs", None),
            P("cells", None, None, None),
        ),
        out_specs=(P(None, "cells", "obs", None), P(None, "cells")),
        check_vma=False,
    )
```

```python
import jax
import jax.numpy as jnp
from jax import lax
from jax.experimental import pallas as pl
from jax.experimental.pallas import tpu as pltpu
from jax.sharding import PartitionSpec as P


TILE = 128
COMP = 5
CAP = 32
SMOOTHING = 0.25
F32 = jnp.float32
BF16 = jnp.bfloat16
NT = (((1,), (1,)), ((), ()))
FIRST_CELL = 79
FIRST_GROUP = 2

VMEM = pl.BlockSpec(memory_space=pltpu.MemorySpace.VMEM)
SMEM = pl.BlockSpec(memory_space=pltpu.MemorySpace.SMEM)
ANY = pl.BlockSpec(memory_space=pl.ANY)


def iota(shape, dim):
    return lax.broadcasted_iota(jnp.int32, shape, dim)


def order(block_ref, cell_ref, same_ref, slot_ref, line_ref):
    chunks, width = block_ref.shape
    blocks = 128
    mark = jnp.where((iota((width, 2 * width), 0) < iota((width, 2 * width), 1)), 1.0, 0.0).astype(BF16)
    line_ref[...] = cell_ref[...].astype(F32)
    named = (iota((blocks, width), 0) + FIRST_CELL) % blocks
    before = jnp.zeros((blocks, width), F32)
    for j in range(chunks):
        same = named == block_ref[j : j + 1, :]
        marked = jnp.where(same, 1.0, 0.0).astype(BF16)
        same_ref[j] = marked
        counted = jnp.dot(marked, mark, preferred_element_type=F32)
        rank = jnp.sum(jnp.where(same, counted[:, :width] + before, 0.0), axis=0, keepdims=True)
        slot_ref[j] = jnp.where(iota((CAP, width), 0).astype(F32) == rank, 1.0, 0.0).astype(BF16)
        before = before + counted[:, width:]


def project(
    hist_hbm, ret_hbm, adj_hbm, weight_hbm, amp_hbm, block_hbm, cell_hbm, step_hbm,
    out_ref, inner_ref, outer_ref, adj_ref, step_ref, same_ref, slot_ref, cell_line_ref,
    hist_ref, ret_ref, weight_ref, amp_ref, block_ref, cell_ref, part_ref, sems,
):
    group = lax.axis_index("obs")
    odd = lax.axis_index("cells") % 2
    copies = out_ref.shape[0]
    tiles, observers = ret_hbm.shape
    azimuths, radii = adj_ref.shape[1:3]
    count = COMP * tiles
    half = tiles * TILE // 2
    moves = [
        pltpu.make_async_copy(source, target, sems.at[i])
        for i, (source, target) in enumerate(
            (
                (hist_hbm, hist_ref),
                (ret_hbm, ret_ref),
                (adj_hbm, adj_ref),
                (weight_hbm.at[:half], weight_ref.at[:half]),
                (amp_hbm.at[:, :, :half], amp_ref.at[:, :, :half]),
                (weight_hbm.at[half:], weight_ref.at[half:]),
                (amp_hbm.at[:, :, half:], amp_ref.at[:, :, half:]),
                (block_hbm, block_ref),
                (cell_hbm, cell_ref),
                (step_hbm, step_ref),
            )
        )
    ]
    for move in moves:
        move.start()
    moves[0].wait()
    moves[1].wait()
    hist = hist_ref[...].astype(F32)
    rows = tiles * observers
    column = [jnp.concatenate([hist[:, j * 128 : (j + 1) * 128]] * tiles, axis=0) for j in range(3)]
    eye = iota((observers, observers), 0) == iota((observers, observers), 1)
    shift = jnp.concatenate(
        [
            jnp.broadcast_to(
                jnp.sum(jnp.where(eye, ret_ref[t : t + 1, :].astype(F32), 0.0), axis=1, keepdims=True), (observers, 128)
            )
            for t in range(tiles)
        ],
        axis=0,
    ).astype(jnp.int32)
    lane = iota((rows, 128), 1)
    far = shift >= 128
    column = [
        jnp.where(far, column[1], column[0]),
        jnp.where(far, column[2], column[1]),
        column[2],
    ]
    for amount in (64, 32, 16, 8, 4, 2, 1):
        rolled = [pltpu.roll(x, 128 - amount, 1) for x in column]
        stays = lane < 128 - amount
        chosen = (shift & amount) != 0
        column = [
            jnp.where(chosen, jnp.where(stays, rolled[0], rolled[1]), column[0]),
            jnp.where(chosen, jnp.where(stays, rolled[1], rolled[2]), column[1]),
            jnp.where(chosen, rolled[2], column[2]),
        ]
    window = jnp.concatenate(column[:2], axis=1).astype(BF16)
    moves[2].wait()
    for c in range(COMP):
        for a in range(azimuths):
            place = count + c * azimuths + a
            for copy in range(copies):
                up = jnp.full((1, 128), (copy + FIRST_GROUP) % copies, jnp.int32) > group
                out_ref[copy, place : place + 1, :] = jnp.where(
                    up, adj_ref[c, a, radii - 1 : radii, :], adj_ref[c, a, 0:1, :]
                )
    for copy in range(copies):
        out_ref[copy, count + 10 : count + 16, :] = jnp.zeros((6, 128), F32)
    even = odd == 0
    inner_ref[...] = jnp.where(even, adj_ref[:, azimuths - 1], adj_ref[:, 0])
    outer_ref[...] = jnp.where(even, adj_ref[:, 0], adj_ref[:, azimuths - 1])
    moves[7].wait()
    moves[8].wait()
    order(block_ref, cell_ref, same_ref, slot_ref, cell_line_ref)
    for t in range(tiles):
        if t == 0:
            moves[3].wait()
            moves[4].wait()
        if t == tiles // 2:
            moves[5].wait()
            moves[6].wait()
        span = slice(t * TILE, (t + 1) * TILE)
        projected = lax.dot_general(
            window[t * observers : (t + 1) * observers],
            weight_ref[span, :],
            NT,
            preferred_element_type=F32,
        )
        for c in range(COMP):
            part_ref[c * tiles + t : c * tiles + t + 1, :] = jnp.sum(
                amp_ref[c, :, span].astype(F32) * projected, axis=0, keepdims=True
            )
    for copy in range(copies):
        out_ref[copy, :count, :] = part_ref[...]
    moves[9].wait()


def whole_source(part_ref, count):
    source = part_ref[0, :count, :]
    for group in range(1, part_ref.shape[0]):
        source = source + part_ref[group, :count, :]
    return source


def pack(part_ref, same_ref, slot_ref, line_ref, out_ref):
    chunks, width = line_ref.shape
    lines = jnp.concatenate([whole_source(part_ref, COMP * chunks), line_ref[...]], axis=0)
    high = lines.astype(BF16).astype(F32)
    low = lines - high
    total = jnp.zeros((128, (COMP + 1) * CAP), F32)
    for j in range(chunks):
        slot = slot_ref[j]
        placed = []
        for part in (high, low):
            placed.append(
                jnp.concatenate(
                    [
                        jnp.broadcast_to(part[c * chunks + j : c * chunks + j + 1, :], (CAP, width)).astype(BF16) * slot
                        for c in range(COMP + 1)
                    ],
                    axis=0,
                )
            )
        same = same_ref[j]
        total = total + lax.dot_general(
            jnp.concatenate([same, same], axis=1),
            jnp.concatenate(placed, axis=1),
            NT,
            preferred_element_type=F32,
        )
    rest = jnp.concatenate([total[:, 128:], jnp.zeros((128, 64), F32)], axis=1)
    out_ref[:, 0, :] = jnp.concatenate([total[:, :128], rest], axis=1)


def stencil(part_ref, adj_ref, step_ref, jac_ref, out_ref, source_ref, mix_ref):
    chunks = source_ref.shape[1] // TILE
    source = whole_source(part_ref, COMP * chunks)
    for c in range(COMP):
        for j in range(chunks):
            source_ref[c : c + 1, j * TILE : (j + 1) * TILE] = source[c * chunks + j : c * chunks + j + 1, :]
    group = lax.axis_index("obs")
    groups = part_ref.shape[0]
    azimuths, radii, length = adj_ref.shape[1:]
    row = iota((radii, length), 0)
    lane = iota((radii, length), 1)
    below = jnp.maximum(group - 1, 0)
    above = jnp.minimum(group + 1, groups - 1)
    has_below = jnp.where(group > 0, 1.0, 0.0)
    has_above = jnp.where(group < groups - 1, 1.0, 0.0)
    for k in range(COMP):
        for c in range(COMP):
            mix_ref[k * COMP + c : k * COMP + c + 1, :] = jnp.full((1, length), 0.5 * jac_ref[0, k, 0, c], F32)
    none = jnp.zeros((radii, length), F32)
    uppers = part_ref[(above - FIRST_GROUP + groups) % groups, 40:56, :] * has_above
    lowers = part_ref[(below - FIRST_GROUP + groups) % groups, 40:56, :] * has_below
    for a in range(azimuths):
        centre = [adj_ref[c, a] for c in range(COMP)]
        pairs = [[], [], []]
        for c in range(COMP):
            x = centre[c]
            ahead = none if a == azimuths - 1 else adj_ref[c, a + 1]
            behind = none if a == 0 else adj_ref[c, a - 1]
            pairs[0].append((ahead, behind))
            place = c * azimuths + a
            upper = uppers[place : place + 1]
            lower = lowers[place : place + 1]
            pairs[1].append(
                (
                    jnp.where(row == radii - 1, upper, pltpu.roll(x, radii - 1, 0)),
                    jnp.where(row == 0, lower, pltpu.roll(x, 1, 0)),
                )
            )
            pairs[2].append(
                (
                    jnp.where(lane == length - 1, 0.0, pltpu.roll(x, length - 1, 1)),
                    jnp.where(lane == 0, 0.0, pltpu.roll(x, 1, 1)),
                )
            )
        differences = [[f - b for f, b in pairs[d]] for d in range(3)]
        for c in range(COMP):
            rotated = jnp.zeros((radii, length), F32)
            spread = -6.0 * centre[c]
            for d in range(3):
                spread = spread + (pairs[d][c][0] + pairs[d][c][1])
                for k in range(COMP):
                    rotated = rotated + jac_ref[d, k, 0, c] * differences[d][k]
            summed = 0.5 * rotated + SMOOTHING * spread
            out_ref[c, a] = centre[c] + step_ref[a] * summed


def land(got_ref, base_ref, inner_ref, outer_ref, step_ref, mix_ref, source_ref, out_ref, source_hbm, sem):
    move = pltpu.make_async_copy(source_ref, source_hbm, sem)
    move.start()
    group = lax.axis_index("obs")
    azimuths, radii, length = base_ref.shape[1:]
    radii_all = radii * lax.axis_size("obs")
    got = jnp.concatenate([got_ref[:, :128].T, got_ref[:, 128:].T], axis=0)
    sources = got_ref.shape[0]
    high = got.astype(BF16).astype(F32)
    low = got - high
    cell = got[COMP * CAP : (COMP + 1) * CAP].astype(jnp.int32)
    cell_row = (cell // length % radii_all).astype(F32)
    cell_column = (cell // (length * radii_all) * length + cell % length).astype(F32)
    wanted = (iota((radii, sources), 0) + group * radii).astype(F32).astype(BF16)
    columns = azimuths * length
    column = iota((columns, sources), 0).astype(F32).astype(BF16)
    one, none = jnp.ones((), BF16), jnp.zeros((), BF16)
    total = jnp.zeros((2 * COMP * radii, columns), F32)
    for first in range(0, CAP, 2):
        values, places = [], []
        for k in range(first, first + 2):
            row = jnp.broadcast_to(cell_row[k : k + 1], wanted.shape).astype(BF16)
            here = jnp.where(wanted == row, one, none)
            values.append(
                jnp.concatenate(
                    [
                        jnp.broadcast_to(part[c * CAP + k : c * CAP + k + 1], wanted.shape).astype(BF16) * here
                        for part in (high, low)
                        for c in range(COMP)
                    ],
                    axis=0,
                )
            )
            at = jnp.broadcast_to(cell_column[k : k + 1], column.shape).astype(BF16)
            places.append(jnp.where(column == at, one, none))
        total = total + lax.dot_general(
            jnp.concatenate(values, axis=1), jnp.concatenate(places, axis=1), NT, preferred_element_type=F32
        )
    half = COMP * radii
    even = lax.axis_index("cells") % 2 == 0
    behind = jnp.where(even, outer_ref[...], inner_ref[...])
    ahead = jnp.where(even, inner_ref[...], outer_ref[...])
    for c in range(COMP):
        mix = [mix_ref[k * COMP + c : k * COMP + c + 1, :] for k in range(COMP)]
        spills = [jnp.zeros((radii, length), F32)] * azimuths
        spills[0] = spills[0] + SMOOTHING * behind[c] - sum(mix[k] * behind[k] for k in range(COMP))
        spills[-1] = spills[-1] + SMOOTHING * ahead[c] + sum(mix[k] * ahead[k] for k in range(COMP))
        for a in range(azimuths):
            rows = slice(c * radii, (c + 1) * radii)
            lower = slice(half + c * radii, half + (c + 1) * radii)
            span = slice(a * length, (a + 1) * length)
            out_ref[c, a] = base_ref[c, a] + step_ref[a] * spills[a] + (total[rows, span] + total[lower, span])
    move.wait()


def turned(size, first):
    return [[(i + first) % size for i in range(size)]]


def near(x):
    return pltpu.with_memory_space_constraint(x, pltpu.VMEM)


def on_device(
    histories, amplitude, weights, retarded, owner_block, owner_cell, adjoint, step_size, jacobian
):
    groups = lax.axis_size("obs")
    count = lax.axis_size("cells")
    panels = weights.shape[0]
    chunks = panels // TILE
    blocks2 = owner_block.reshape(chunks, TILE)
    cells2 = owner_cell.reshape(chunks, TILE)
    amp = amplitude.transpose(1, 0, 2)
    edge = pltpu.VMEM((COMP,) + adjoint.shape[2:], F32)

    partial_copies, inner, outer, adjoint_near, step_near, same, slot, lines = pl.pallas_call(
        project,
        out_shape=(
            pltpu.VMEM((groups, 56, TILE), F32),
            edge,
            edge,
            pltpu.VMEM(adjoint.shape, F32),
            pltpu.VMEM(step_size.shape, F32),
            pltpu.VMEM((chunks, 128, TILE), BF16),
            pltpu.VMEM((chunks, CAP, TILE), BF16),
            pltpu.VMEM((chunks, TILE), F32),
        ),
        in_specs=[ANY] * 8,
        out_specs=(VMEM,) * 8,
        scratch_shapes=[
            pltpu.VMEM(histories.shape, BF16),
            pltpu.VMEM((chunks, histories.shape[0]), jnp.int32),
            pltpu.VMEM(weights.shape, BF16),
            pltpu.VMEM(amp.shape, BF16),
            pltpu.VMEM(blocks2.shape, jnp.int32),
            pltpu.VMEM(cells2.shape, jnp.int32),
            pltpu.VMEM((COMP * chunks, TILE), F32),
            pltpu.SemaphoreType.DMA((10,)),
        ],
        name="project",
    )(histories, retarded.T, adjoint, weights, amp, blocks2, cells2, step_size)
    parts = lax.all_to_all(
        partial_copies, "obs", 0, 0, axis_index_groups=turned(groups, FIRST_GROUP), tiled=True
    )
    inner = lax.ppermute(inner, "cells", [(i, i ^ 1) for i in range(count)])
    outer = lax.ppermute(outer, "cells", [(i, ((i + 1 ^ 1) - 1) % count) for i in range(count)])

    outgoing = pl.pallas_call(
        pack,
        out_shape=jax.ShapeDtypeStruct((count, 1, 256), F32),
        in_specs=[VMEM] * 4,
        out_specs=VMEM,
        name="pack",
    )(near(parts), near(same), near(slot), near(lines))
    received = lax.all_to_all(
        outgoing, "cells", 0, 0, axis_index_groups=turned(count, FIRST_CELL), tiled=True
    )

    base, source, mix = pl.pallas_call(
        stencil,
        out_shape=(
            pltpu.VMEM(adjoint.shape, F32),
            pltpu.VMEM((COMP, panels), F32),
            pltpu.VMEM((32, adjoint.shape[3]), F32),
        ),
        in_specs=[VMEM] * 3 + [SMEM],
        out_specs=(VMEM, VMEM, VMEM),
        name="stencil",
    )(near(parts), near(adjoint_near), near(step_near), jacobian.transpose(1, 2, 0, 3))
    adjoint_next, panel_source = pl.pallas_call(
        land,
        out_shape=(
            jax.ShapeDtypeStruct(adjoint.shape, F32),
            jax.ShapeDtypeStruct((COMP, panels), F32),
        ),
        in_specs=[VMEM] * 7,
        out_specs=(VMEM, ANY),
        scratch_shapes=[pltpu.SemaphoreType.DMA],
        name="land",
    )(near(received.reshape(count, 256)), near(base), near(inner), near(outer), near(step_near), near(mix), near(source))
    return adjoint_next, panel_source


def solution(mesh):
    return jax.shard_map(
        on_device,
        mesh=mesh,
        in_specs=(
            P("obs", None),
            P("obs", None, "cells"),
            P("cells", None),
            P("obs", "cells"),
            P("cells"),
            P("cells"),
            P(None, "cells", "obs", None),
            P("cells", "obs", None),
            P("cells", None, None, None),
        ),
        out_specs=(P(None, "cells", "obs", None), P(None, "cells")),
        check_vma=False,
    )
```
